128 devices in a mesh: grp: 8 (over x, core), ex: 16 (over z, y).
Axes of the slice: x: 4, y: 4, z: 4, core: 2. Of those that a mesh axis runs over, the one named last changes fastest.
Arguments:
- item_ids: int32 [256, 256], P(('grp', 'ex')), may hold values from 0 to 65535, as said below
- lengths: int32 [256], P(('grp', 'ex')), may hold values from 32 to 256
- expert_ids: int32 [65536, 2], P(('grp', 'ex')), may hold values from 0 to 31, all different within a row; in each aligned block of 512 rows (0 to 511, 512 to 1023, ...) at most 48 rows name the same one
- gate_weights: float32 [65536, 2], P(('grp', 'ex')), may hold values from 0.1 to 1
- table: bfloat16 [65536, 512], P('ex'), may hold values from -6 to 6
- norm_gain: float32 [512], replicated, may hold values from 0.1 to 1.9
- w_gate: bfloat16 [32, 512, 1024], P('ex'), may hold values from -0.25 to 0.25
- w_up: bfloat16 [32, 512, 1024], P('ex'), may hold values from -0.25 to 0.25
- w_down: bfloat16 [32, 512, 1024], P('ex'), may hold values from -0.1875 to 0.1875
- d_out: bfloat16 [65536, 512], P(('grp', 'ex')), may hold values from -0.59765625 to 0.59765625
Outputs:
- layer_out: bfloat16 [65536, 512], P(('grp', 'ex'))
- grad_gate: float32 [32, 512, 1024], P('ex', None, 'grp')
- grad_up: float32 [32, 512, 1024], P('ex', None, 'grp')
- grad_down: float32 [32, 512, 1024], P('ex', None, 'grp')
The draws below stay inside these ranges and needn't reach their ends.
Inputs may be any that keep to these rules, and one draw needn't show every extreme that they name: `item_ids`: split the ids into blocks of 4096 consecutive values. Among the 512 positions of each aligned run of 2 sequences, at most 128 name ids of one such block, and in every such run some block is named exactly 128 times. `expert_ids`: each token names 2 different experts. Within each aligned block of 512 tokens no expert is named more than 48 times, and in some block some expert is named exactly 48 times.
All inputs are finite; a program needn't handle non-finite values.
Results may differ from the reference program's by a relative error of at most 0.012.
Values may be sent and summed in bfloat16 or wider, within the bound.
No kernel may reach another device: no remote copies, remote signals or barrier semaphores. Data moves between devices by JAX's collectives and lax.ppermute only.
A program may use at most 128 MiB of HBM per device.

```python
import math
import jax
import jax.numpy as jnp
import numpy as np
from jax import lax

D = 512
FF = 1024
EXPERTS = 32
TOP = 2
SEQ = 256
ROWS_DEV = 4096
SEQS_DEV = 2
TOK_DEV = 512
ROW_CAP = 128
SEQUENCES = 256
TOKENS = 65536
VOCAB = 65536
CAP = 48
N_GRP = 8
N_EX = 16


def draw_item_ids(key, part):
    blocks = SEQUENCES // SEQS_DEV
    key_hot, key_perm, key_raw, key_span = jax.random.split(jax.random.fold_in(key, 4127), 4)
    hot = (jax.random.permutation(key_hot, blocks) % N_EX).astype(jnp.int32)
    within = jnp.arange(TOK_DEV, dtype=jnp.int32)

    def block_ids(hot_shard, perm_key, raw_key, span_key):
        others = (hot_shard + 1 + (within - ROW_CAP) % (N_EX - 1)) % N_EX
        shard = jnp.where(within < ROW_CAP, hot_shard, others)
        span = jax.random.randint(span_key, (TOK_DEV,), 1, ROWS_DEV + 1)
        raw = jax.random.randint(raw_key, (TOK_DEV,), 0, ROWS_DEV) % span
        row = (raw * 2897 + 1013) % ROWS_DEV
        row = jnp.where(within == 0, ROWS_DEV - 1, jnp.where(within == 1, 0, row))
        ids = (shard * ROWS_DEV + row).astype(jnp.int32)
        return ids[jax.random.permutation(perm_key, TOK_DEV)]
    result = jax.vmap(block_ids)(hot, jax.random.split(key_perm, blocks), jax.random.split(key_raw, blocks), jax.random.split(key_span, blocks))
    return result.reshape(SEQUENCES, SEQ).astype(jnp.int32)


def with_ends(values, rng, least, largest):
    index_at = [jax.random.randint(jax.random.fold_in(rng, axis), (), 0, length) for axis, length in enumerate(values.shape)]
    main_axis = values.shape.index(max(values.shape))
    next_to = index_at[:main_axis] + [(index_at[main_axis] + 1) % values.shape[main_axis]] + index_at[main_axis + 1:]
    return values.at[tuple(index_at)].set(least).at[tuple(next_to)].set(largest)


def levels(own_key, extent, pieces, least, largest):
    level = 1.0
    for dim, blocks in pieces:
        draws = jax.random.uniform(jax.random.fold_in(jax.random.fold_in(own_key, 6), dim), (blocks,), jnp.float32, least / len(pieces), largest / len(pieces))
        level = level * jnp.repeat(jnp.exp(draws), extent[dim] // blocks).reshape((-1,) + (1,) * (len(extent) - 1 - dim))
    return level


def routed_block(stream_key, own, number, rows, count, top, reach, skew):
    order = jax.random.permutation(stream_key, count)
    heavy_load, common = portions_of(count, rows * top, reach, skew, True), portions_of(count, rows * top, reach, skew, False)
    places = jnp.arange(count)

    def named(sizes, rotation):
        used = int((sizes > 0).sum())
        fixed = max(1, used // 4)
        passed = fixed + (places - fixed + rotation * (used - fixed)) % max(1, count - fixed)
        return jnp.zeros((count,), jnp.int32).at[order[jnp.where(places < fixed, places, passed)]].set(jnp.asarray(sizes, jnp.int32))

    sizes = jnp.where(number % 4 == 0, named(heavy_load, number // 4), named(common, number - number // 4 - 1))
    mixed = jax.random.permutation(jax.random.fold_in(own, 3), count)
    source_of, sink = mixed[0:count // 2 * 2:2], mixed[1:count // 2 * 2:2]
    slack = jnp.minimum(sizes[source_of] - 1, reach - sizes[sink]) // 2
    slack = jnp.where((source_of == order[0]) | (sink == order[0]) | (sizes[sink] == 0), 0, jnp.maximum(slack, 0))
    passed = jax.random.randint(jax.random.fold_in(own, 4), (count // 2,), 0, 1 << 20) % (slack + 1)
    sizes = sizes.at[source_of].add(-passed).at[sink].add(passed)
    labels = jnp.searchsorted(jnp.cumsum(sizes), jnp.arange(rows * top), side="right").astype(jnp.int32)
    listing = labels.reshape(top, rows).T
    listing = listing[jax.random.permutation(jax.random.fold_in(own, 1), rows)]
    rotation = jax.random.randint(jax.random.fold_in(own, 2), (rows, 1), 0, top)
    return jnp.take_along_axis(listing, (jnp.arange(top)[None, :] + rotation) % top, axis=1)


def portions_of(number_of, total, reach, skew, full):
    loads = [(1 << 20) // math.isqrt(standing ** skew) + 1 for standing in range(1, number_of + 1)]
    largest = reach if full else min(reach, max(-(-total // number_of), total * loads[0] // sum(loads)))
    least = 1 if total - largest >= number_of - 1 else 0
    holding, surplus = [largest] + [least] * (number_of - 1), total - largest - least * (number_of - 1)
    while surplus > 0:
        candidates = [i for i in range(1, number_of) if holding[i] < largest] or [i for i in range(1, number_of) if holding[i] < reach]
        pool, remaining = sum([loads[i] for i in candidates]), surplus
        for i in candidates:
            more = min(reach - holding[i], max(1, remaining * loads[i] // pool), surplus)
            holding[i] = holding[i] + more
            surplus = surplus - more
    return np.array(holding)


def noise(stream_key, shape, deviation, reach, cuts=(), kind=jnp.bfloat16):
    entries = jax.random.normal(stream_key, shape, jnp.float32) * deviation
    if len(cuts) > 0:
        entries = levels(stream_key, shape, cuts, -0.22, 0.18) * entries
    return jnp.clip(entries, min=-reach, max=reach).astype(kind)


def setup_inputs(seed: int = 0) -> dict:
    key_of = jax.random.split(jax.random.key(seed), 11)
    item_ids = draw_item_ids(jax.random.fold_in(key_of[10], 71), 0)
    lengths = with_ends(jax.random.randint(key_of[1], (SEQUENCES,), SEQ // 8, SEQ + 1), jax.random.fold_in(key_of[1], 1), SEQ // 8, SEQ).astype(jnp.int32)
    expert_ids_keys = jax.random.split(jax.random.fold_in(key_of[2], 1), TOKENS // TOK_DEV)
    expert_ids_turns = jax.random.permutation(jax.random.fold_in(key_of[2], 3), TOKENS // TOK_DEV)
    expert_ids = jax.vmap(lambda own, number: routed_block(jax.random.fold_in(key_of[2], 2), own, number, TOK_DEV, EXPERTS, TOP, CAP, 2))(expert_ids_keys, expert_ids_turns).reshape((TOKENS, TOP))
    gate_weights = jnp.clip(0.1 + 0.9 * jax.random.uniform(key_of[3], (TOKENS, TOP), jnp.float32) ** levels(key_of[3], (TOKENS, TOP), ((0, 128),), -0.2, 0.2), 0.1, 1.0)
    table = noise(key_of[4], (VOCAB, D), 1.0, 6.0, ((0, 16),))
    norm_gain = jnp.clip(1.0 + 0.18 * jax.random.normal(key_of[5], (D,), jnp.float32), 0.1, 1.9)
    w_gate = noise(key_of[6], (EXPERTS, D, FF), D ** -0.5, 0.25, ((0, 16),))
    w_up = noise(key_of[7], (EXPERTS, D, FF), D ** -0.5, 0.25, ((0, 16),))
    w_down = noise(key_of[8], (EXPERTS, D, FF), FF ** -0.5, 0.1875, ((0, 16),))
    d_out = noise(key_of[9], (TOKENS, D), 0.1, 0.59765625, ((0, 128),))
    return {"item_ids": item_ids, "lengths": lengths, "expert_ids": expert_ids, "gate_weights": gate_weights, "table": table, "norm_gain": norm_gain, "w_gate": w_gate, "w_up": w_up, "w_down": w_down, "d_out": d_out}


EPSILON = 1e-06

def reference(item_ids, lengths, expert_ids, gate_weights, table, norm_gain, w_gate, w_up, w_down, d_out):
    flat_ids = item_ids.reshape(-1).astype(jnp.int32)
    position = lax.broadcasted_iota(jnp.int32, item_ids.shape, 1)
    valid = (position < lengths[:, None]).reshape(-1)
    looked = jnp.take(table, flat_ids, axis=0).astype(jnp.float32)
    embedded = jnp.where(valid[:, None], looked, jnp.zeros_like(looked))
    mean_square = lax.optimization_barrier(jnp.mean(embedded * embedded, axis=1, keepdims=True))
    normed = (embedded * lax.rsqrt(mean_square + EPSILON) * norm_gain[None, :]).astype(jnp.bfloat16)
    cotangent = (gate_weights[:, :, None] * d_out[:, None, :].astype(jnp.float32)).astype(jnp.bfloat16)
    blocks = N_GRP * N_EX
    pair_expert = expert_ids.reshape(blocks, TOK_DEV * TOP).astype(jnp.int32)
    expert_iota = lax.broadcasted_iota(jnp.int32, (1, 1, EXPERTS), 2)
    onehot = (pair_expert[:, :, None] == expert_iota).astype(jnp.int32)
    rank = lax.optimization_barrier(jnp.sum((jnp.cumsum(onehot, axis=1) - onehot) * onehot, axis=2))
    source = lax.broadcasted_iota(jnp.int32, (blocks, 1), 0) % N_EX
    slots = (pair_expert * N_EX + source) * CAP + rank
    group_tokens = N_EX * TOK_DEV
    slots = slots.reshape(N_GRP, group_tokens, TOP)
    span = N_EX * CAP

    def one_expert(operands):
        rows_in, cot_in, gate_w, up_w, down_w = operands
        gate_pre = jnp.dot(rows_in, gate_w, preferred_element_type=jnp.float32)
        up_pre = jnp.dot(rows_in, up_w, preferred_element_type=jnp.float32)
        sigmoid = jax.nn.sigmoid(gate_pre)
        silu_gate = gate_pre * sigmoid
        active = (silu_gate * up_pre).astype(jnp.bfloat16)
        expert_out = jnp.dot(active, down_w.T, preferred_element_type=jnp.float32).astype(jnp.bfloat16)
        d_active = jnp.dot(cot_in, down_w, preferred_element_type=jnp.float32)
        d_gate = (d_active * up_pre * sigmoid * (1.0 + gate_pre * (1.0 - sigmoid))).astype(jnp.bfloat16)
        d_up = (d_active * silu_gate).astype(jnp.bfloat16)
        part_gate = jnp.dot(rows_in.T, d_gate, preferred_element_type=jnp.float32).astype(jnp.bfloat16)
        part_up = jnp.dot(rows_in.T, d_up, preferred_element_type=jnp.float32).astype(jnp.bfloat16)
        part_down = jnp.dot(cot_in.T, active, preferred_element_type=jnp.float32).astype(jnp.bfloat16)
        return (expert_out, part_gate, part_up, part_down)

    def one_group(carry, inputs):
        group_normed, group_cot, group_slots, group_embedded, group_gates = inputs
        empty = jnp.zeros((EXPERTS * span, D), jnp.bfloat16)
        buffer_rows = empty.at[group_slots].set(jnp.broadcast_to(group_normed[:, None, :], (group_tokens, TOP, D)))
        buffer_cot = empty.at[group_slots].set(group_cot)
        outs, part_gate, part_up, part_down = lax.map(one_expert, (buffer_rows.reshape(EXPERTS, span, D), buffer_cot.reshape(EXPERTS, span, D), w_gate, w_up, w_down))
        picked = jnp.take(outs.reshape(EXPERTS * span, D), group_slots, axis=0)
        mixed = group_embedded + lax.optimization_barrier(jnp.sum(group_gates[:, :, None] * picked.astype(jnp.float32), axis=1))
        parts = lax.optimization_barrier((part_gate, part_up, part_down))
        carry = (carry[0] + parts[0].astype(jnp.float32), carry[1] + parts[1].astype(jnp.float32), carry[2] + parts[2].astype(jnp.float32))
        return (carry, mixed.astype(jnp.bfloat16))
    zeros = jnp.zeros((EXPERTS, D, FF), jnp.float32)
    inputs = (normed.reshape(N_GRP, group_tokens, D), cotangent.reshape(N_GRP, group_tokens, TOP, D), slots, embedded.reshape(N_GRP, group_tokens, D), gate_weights.reshape(N_GRP, group_tokens, TOP))
    grads, mixed = lax.scan(one_group, (zeros, zeros, zeros), inputs)
    return (mixed.reshape(TOKENS, D), grads[0], grads[1], grads[2])
```

```python
import jax
import jax.numpy as jnp
from jax import lax
from jax.experimental import pallas as pl
from jax.experimental.pallas import tpu as pltpu
from jax.sharding import PartitionSpec as P

TOP = 2
CAP = 48
ROW_CAP = 128
EPSILON = 1e-06
BF = jnp.bfloat16
F32 = jnp.float32
I32 = jnp.int32


def dot(a, b, dims=((1,), (0,))):
    return lax.dot_general(a, b, (dims, ((), ())), preferred_element_type=F32)


def ones_where(mask):
    return jnp.where(mask, 1.0, 0.0).astype(BF)


def shape(dims, dtype):
    return jax.ShapeDtypeStruct(dims, dtype)


def call(body, out_shape, name, **kw):
    return pl.pallas_call(
        body,
        out_shape=out_shape,
        name=name,
        compiler_params=pltpu.CompilerParams(vmem_limit_bytes=56 * 1024 * 1024),
        **kw,
    )


def index_body(len_ref, ids_ref, exp_ref, gw_ref, req_ref, rows_ref, cols_ref):
    seqs, seq_len = ids_ref.shape
    tok = seqs * seq_len
    blocks = req_ref.shape[0]
    experts = 32
    ids = jnp.concatenate([ids_ref[i : i + 1, :] for i in range(seqs)], axis=1)
    upper = ones_where(
        lax.broadcasted_iota(I32, (tok, tok), 0) < lax.broadcasted_iota(I32, (tok, tok), 1)
    )
    low = ids % 4096
    block = ids // 4096
    in_block = lax.broadcasted_iota(I32, (blocks, tok), 0) == block
    e0 = exp_ref[0:1, :]
    e1 = exp_ref[1:2, :]
    expert_iota = lax.broadcasted_iota(I32, (experts, tok), 0)
    hot0 = expert_iota == e0
    hot1 = expert_iota == e1
    cum_b = dot(ones_where(in_block), upper)
    cum_e = dot(ones_where(jnp.logical_or(hot0, hot1)), upper)
    rank_b = jnp.sum(jnp.where(in_block, cum_b, 0.0), axis=0, keepdims=True).astype(I32)
    rank0 = jnp.sum(jnp.where(hot0, cum_e, 0.0), axis=0, keepdims=True).astype(I32)
    rank1 = jnp.sum(jnp.where(hot1, cum_e, 0.0), axis=0, keepdims=True).astype(I32)
    at_rank = ones_where(lax.broadcasted_iota(I32, (ROW_CAP, tok), 0) == rank_b)
    high6 = jnp.where(in_block, (low // 64).astype(F32), 0.0).astype(BF)
    low6 = jnp.where(in_block, (low % 64).astype(F32), 0.0).astype(BF)
    nt = ((1,), (1,))
    req_ref[...] = (dot(high6, at_rank, nt) * 64.0 + dot(low6, at_rank, nt)).astype(I32)
    slot_b = block * ROW_CAP + rank_b
    slot0 = e0 * CAP + rank0
    slot1 = e1 * CAP + rank1
    position = lax.broadcasted_iota(I32, (1, seq_len), 1)
    valid = jnp.concatenate(
        [jnp.where(position < len_ref[i], 1, 0) for i in range(seqs)], axis=1
    )
    zero = jnp.zeros((1, tok), F32)
    rows = jnp.concatenate(
        [
            slot_b.astype(F32),
            valid.astype(F32),
            slot0.astype(F32),
            slot1.astype(F32),
            gw_ref[0:1, :],
            gw_ref[1:2, :],
            zero,
            zero,
        ],
        axis=0,
    )
    rows_ref[...] = rows
    cols_ref[...] = rows.T


def spread(rows, slots):
    at = lax.broadcasted_iota(I32, (slots, rows.shape[1]), 0).astype(F32)
    return at == rows[2:3, :], at == rows[3:4, :]


def cot_body(rows_ref, d_ref, out_ref):
    slots = out_ref.shape[0]
    rows = rows_ref[...]
    d = d_ref[...]
    step = 512
    for s in range(0, slots, step):
        at = lax.broadcasted_iota(I32, (step, rows.shape[1]), 0).astype(F32) + float(s)
        m0 = at == rows[2:3, :]
        m1 = at == rows[3:4, :]
        moved = dot(ones_where(jnp.logical_or(m0, m1)), d)
        weight = jnp.sum(
            jnp.where(m0, rows[4:5, :], jnp.where(m1, rows[5:6, :], 0.0)), axis=1, keepdims=True
        )
        out_ref[s : s + step, :] = (weight * moved).astype(BF)


def norm_body(rows_ref, cols_ref, gain_ref, got_ref, emb_ref, out_ref):
    tok = emb_ref.shape[0]
    slots = out_ref.shape[0]
    cols = cols_ref[...]
    rows = rows_ref[...]
    pick = ones_where(
        lax.broadcasted_iota(I32, (tok, got_ref.shape[0]), 1).astype(F32) == cols[:, 0:1]
    )
    embedded = jnp.where(cols[:, 1:2] > 0.0, dot(pick, got_ref[...]), 0.0)
    emb_ref[...] = embedded.astype(BF)
    mean_square = jnp.mean(embedded * embedded, axis=1, keepdims=True)
    normed = (embedded * lax.rsqrt(mean_square + EPSILON) * gain_ref[...]).astype(BF)
    m0, m1 = spread(rows, slots)
    out_ref[...] = dot(ones_where(jnp.logical_or(m0, m1)), normed).astype(BF)


def d_active_body(cot_ref, wd_ref, out_ref):
    cot = cot_ref[...].reshape(out_ref.shape[1], wd_ref.shape[1])
    out_ref[0] = dot(cot, wd_ref[0])


def forward_body(x_ref, wg_ref, wu_ref, wd_ref, da_ref, out_ref, mid_ref):
    rows = da_ref.shape[1]
    src, _, cap, width = x_ref.shape
    x = x_ref[...].reshape(rows, width)
    step = 192
    per = step // cap
    for i in range(rows // step):
        r = slice(i * step, (i + 1) * step)
        gate = dot(x[r], wg_ref[0])
        up = dot(x[r], wu_ref[0])
        sigmoid = jax.nn.sigmoid(gate)
        silu = gate * sigmoid
        active = (silu * up).astype(BF)
        out = dot(active, wd_ref[0], ((1,), (1,))).astype(BF)
        out_ref[i * per : (i + 1) * per, 0] = out.reshape(per, cap, width)
        da = da_ref[0, r]
        d_gate = (da * up * sigmoid * (1.0 + gate * (1.0 - sigmoid))).astype(BF)
        d_up = (da * silu).astype(BF)
        for g in range(8):
            c = slice(g * 128, (g + 1) * 128)
            mid_ref[0, 0, g, r, :] = active[:, c]
            mid_ref[1, 0, g, r, :] = d_gate[:, c]
            mid_ref[2, 0, g, r, :] = d_up[:, c]


def lhs_of(part, cot_ref, x_ref, lt_ref):
    width, rows = lt_ref.shape

    @pl.when(part == 0)
    def _():
        lt_ref[...] = cot_ref[...].reshape(rows, width).T

    @pl.when(part == 1)
    def _():
        lt_ref[...] = x_ref[...].reshape(rows, width).T


def products(lt_ref, d_refs):
    lt = lt_ref[...]
    for i in (0, 2):
        pair = jnp.concatenate([d_refs[i][0, 0, 0], d_refs[i + 1][0, 0, 0]], axis=1)
        got = dot(lt, pair)
        yield i, got[:, :128]
        yield i + 1, got[:, 128:]


def send_body(pre_ref, cot_ref, x_ref, d0, d1, d2, d3, out_ref, lt_ref):
    lhs_of(pl.program_id(0), cot_ref, x_ref, lt_ref)
    for i, block in products(lt_ref, (d0, d1, d2, d3)):
        out_ref[0, i] = block.astype(BF)


def keep_body(pre_ref, cot_ref, x_ref, d0, d1, d2, d3, got_ref, ak, asend, bk, bsend, lt_ref):
    lhs_of(pl.program_id(0), cot_ref, x_ref, lt_ref)
    where_a = {0: (ak, 0), 3: (ak, 1), 1: (asend, 0), 2: (asend, 1)}
    where_b = {0: (bk, 0), 1: (bk, 1), 3: (bsend, 0), 2: (bsend, 1)}
    for i, block in products(lt_ref, (d0, d1, d2, d3)):
        total = (block + got_ref[0, i].astype(F32)).astype(BF)
        half = total.shape[0] // 2
        ref, at = where_a[i]
        ref[0, at] = total[:half]
        ref, at = where_b[i]
        ref[0, at] = total[half:]


def add_body(ak, ar, bk, br, own_a, snd_a, own_b, snd_b):
    for keep, got, own, snd in ((ak, ar, own_a, snd_a), (bk, br, own_b, snd_b)):
        own[...] = keep[:, 0].astype(F32) + got[:, 0].astype(F32)
        snd[...] = (keep[:, 1].astype(F32) + got[:, 1].astype(F32)).astype(BF)


def final_body(*refs):
    ins, (g_down, g_gate, g_up) = refs[:-3], refs[-3:]
    for j in range(2):
        oa, ra, ob, rb = ins[4 * j : 4 * j + 4]
        for part, ref in enumerate((g_down, g_gate, g_up)):
            half = ref.shape[1] // 2
            ref[j, :half] = oa[part] + ra[part].astype(F32)
            ref[j, half:] = ob[part] + rb[part].astype(F32)


def combine_body(cols_ref, emb_ref, ret_ref, out_ref):
    tok = out_ref.shape[0]
    slots = ret_ref.shape[0]
    cols = cols_ref[...]
    ret = ret_ref[...]
    at = lax.broadcasted_iota(I32, (tok, slots), 1).astype(F32)
    first = dot(ones_where(at == cols[:, 2:3]), ret)
    second = dot(ones_where(at == cols[:, 3:4]), ret)
    mixed = emb_ref[...].astype(F32) + (cols[:, 4:5] * first + cols[:, 5:6] * second)
    out_ref[...] = mixed.astype(BF)


def exchange(x):
    return lax.all_to_all(x, "ex", split_axis=0, concat_axis=0, tiled=True)


def on_device(
    item_ids, lengths, expert_ids, gate_weights, table, norm_gain, w_gate, w_up, w_down, d_out
):
    ex_count = lax.axis_size("ex")
    seqs_here, seq_len = item_ids.shape
    tok = seqs_here * seq_len
    width = table.shape[1]
    exp_here, _, ff = w_gate.shape
    slots = exp_here * ex_count * CAP
    rows_e = ex_count * CAP
    vmem = pl.BlockSpec(memory_space=pltpu.VMEM)
    smem = pl.BlockSpec(memory_space=pltpu.SMEM)

    request, rows, cols = call(
        index_body,
        (shape((ex_count, ROW_CAP), I32), shape((8, tok), F32), shape((tok, 8), F32)),
        "index",
        in_specs=[smem, vmem, vmem, vmem],
        out_specs=(vmem, vmem, vmem),
    )(lengths, item_ids, expert_ids.T, gate_weights.T)
    asked = exchange(request)
    send_cot = call(
        cot_body, shape((slots, width), BF), "cot", in_specs=[vmem, vmem], out_specs=vmem
    )(rows, d_out)
    in_cot = exchange(send_cot.reshape(ex_count, exp_here * CAP, width))
    picked = jnp.take(table, asked.reshape(-1), axis=0, mode="clip")
    got = exchange(picked.reshape(ex_count, ROW_CAP, width)).reshape(-1, width)
    embedded, send_rows = call(
        norm_body,
        (shape((tok, width), BF), shape((slots, width), BF)),
        "norm",
        in_specs=[vmem] * 4,
        out_specs=(vmem, vmem),
    )(rows, cols, norm_gain[None, :], got)
    in_rows = exchange(send_rows.reshape(ex_count, exp_here * CAP, width))
    in_cot = in_cot.reshape(ex_count, exp_here, CAP, width)
    in_rows = in_rows.reshape(ex_count, exp_here, CAP, width)
    row_spec = pl.BlockSpec((ex_count, 1, CAP, width), lambda j: (0, j, 0, 0))
    w_spec = pl.BlockSpec((1, width, ff), lambda j: (j, 0, 0))
    da_spec = pl.BlockSpec((1, rows_e, ff), lambda j: (j, 0, 0))
    d_active = call(
        d_active_body,
        shape((exp_here, rows_e, ff), F32),
        "dactive",
        grid=(exp_here,),
        in_specs=[row_spec, w_spec],
        out_specs=da_spec,
    )(in_cot, w_down)
    expert_out, mids = call(
        forward_body,
        (
            shape((ex_count, exp_here, CAP, width), BF),
            shape((3, exp_here, 8, rows_e, 128), BF),
        ),
        "forward",
        grid=(exp_here,),
        in_specs=[row_spec, w_spec, w_spec, w_spec, da_spec],
        out_specs=(row_spec, pl.BlockSpec((3, 1, 8, rows_e, 128), lambda j: (0, j, 0, 0, 0))),
    )(in_rows, w_gate, w_up, w_down, d_active)
    returned = exchange(expert_out.reshape(ex_count, exp_here * CAP, width))

    me = lax.axis_index("grp")
    place = jnp.arange(4, dtype=I32)

    def half_call(j, other, body, extra, extra_specs, outs, out_specs, name):
        pre = jnp.bitwise_xor(me // 2, place) * 2 + jnp.bitwise_xor(me % 2, other)
        row_j = pl.BlockSpec((ex_count, 1, CAP, width), lambda p, pre: (0, j, 0, 0))
        d_specs = [
            pl.BlockSpec(
                (1, 1, 1, rows_e, 128), lambda p, pre, i=i: (p, j, pre[i], 0, 0)
            )
            for i in range(4)
        ]
        return call(
            body,
            outs,
            name,
            grid_spec=pltpu.PrefetchScalarGridSpec(
                num_scalar_prefetch=1,
                grid=(3,),
                in_specs=[row_j, row_j] + d_specs + extra_specs,
                out_specs=out_specs,
                scratch_shapes=[pltpu.VMEM((width, rows_e), BF)],
            ),
        )(pre, in_cot, in_rows, mids, mids, mids, mids, *extra)

    full_spec = pl.BlockSpec((1, 4, width, 128), lambda p, pre: (p, 0, 0, 0))
    half_spec = pl.BlockSpec((1, 2, width // 2, 128), lambda p, pre: (p, 0, 0, 0))
    core = [(g, g ^ 1) for g in range(8)]
    near1 = [(g, g ^ 2) for g in range(8)]
    near3 = [(g, g ^ 6) for g in range(8)]
    crossed = []
    for j in range(exp_here):
        out = half_call(
            j, 1, send_body, (), [], shape((3, 4, width, 128), BF), full_spec, f"send{j}"
        )
        crossed.append(lax.ppermute(out, "grp", core))
    finals = []
    for j in range(exp_here):
        half = shape((3, 2, width // 2, 128), BF)
        ak, asend, bk, bsend = half_call(
            j, 0, keep_body, (crossed[j],), [full_spec], (half,) * 4, (half_spec,) * 4, f"keep{j}"
        )
        ar = lax.ppermute(asend, "grp", near1)
        br = lax.ppermute(bsend, "grp", near3)
        piece = (3, width // 2, 128)
        own_a, snd_a, own_b, snd_b = call(
            add_body,
            (shape(piece, F32), shape(piece, BF)) * 2,
            f"add{j}",
            in_specs=[vmem] * 4,
            out_specs=(vmem,) * 4,
        )(ak, ar, bk, br)
        finals += [own_a, lax.ppermute(snd_a, "grp", near3)]
        finals += [own_b, lax.ppermute(snd_b, "grp", near1)]
    grad = shape((exp_here, width, 128), F32)
    grad_down, grad_gate, grad_up = call(
        final_body, (grad,) * 3, "final", in_specs=[vmem] * 8, out_specs=(vmem,) * 3
    )(*finals)
    output = call(
        combine_body, shape((tok, width), BF), "combine", in_specs=[vmem] * 3, out_specs=vmem
    )(cols, embedded, returned.reshape(slots, width))
    return (output, grad_gate, grad_up, grad_down)


def solution(mesh):
    placed = (
        P(("grp", "ex"), None),
        P(("grp", "ex")),
        P(("grp", "ex"), None),
        P(("grp", "ex"), None),
        P("ex", None),
        P(),
        P("ex", None, None),
        P("ex", None, None),
        P("ex", None, None),
        P(("grp", "ex"), None),
    )
    return jax.shard_map(
        on_device,
        mesh=mesh,
        in_specs=placed,
        out_specs=(
            P(("grp", "ex"), None),
            P("ex", None, "grp"),
            P("ex", None, "grp"),
            P("ex", None, "grp"),
        ),
        check_vma=False,
    )
```

```python
import jax
import jax.numpy as jnp
from jax import lax
from jax.experimental import pallas as pl
from jax.experimental.pallas import tpu as pltpu
from jax.sharding import PartitionSpec as P


CAP = 48
ROW_CAP = 128
EPSILON = 1e-06
BF = jnp.bfloat16
F32 = jnp.float32
I32 = jnp.int32


def dot(a, b, dims=((1,), (0,))):
    return lax.dot_general(a, b, (dims, ((), ())), preferred_element_type=F32)


def ones_where(mask):
    return jnp.where(mask, 1.0, 0.0).astype(BF)


def shape(dims, dtype):
    return jax.ShapeDtypeStruct(dims, dtype)


def stay(*arrays):
    return [pltpu.with_memory_space_constraint(x, pltpu.HBM) for x in arrays]


def call(body, out_shape, mib, **kw):
    return pl.pallas_call(
        body,
        out_shape=out_shape,
        compiler_params=pltpu.CompilerParams(vmem_limit_bytes=mib * 1024 * 1024),
        **kw,
    )


def index_body(len_ref, ids_ref, exp_ref, gw_ref, d_ref, out_ref, rows_ref, cols_ref):
    seqs, seq_len = ids_ref.shape
    tok = seqs * seq_len
    blocks = out_ref.shape[0]
    width = d_ref.shape[1]
    routed = out_ref.shape[1] - 8
    experts = blocks * routed // CAP
    ids = jnp.concatenate([ids_ref[i : i + 1, :] for i in range(seqs)], axis=1)
    upper = ones_where(
        lax.broadcasted_iota(I32, (tok, tok), 0) < lax.broadcasted_iota(I32, (tok, tok), 1)
    )
    low = ids % 4096
    block = ids // 4096
    in_block = lax.broadcasted_iota(I32, (blocks, tok), 0) == block
    e0 = exp_ref[0:1, :]
    e1 = exp_ref[1:2, :]
    expert_iota = lax.broadcasted_iota(I32, (experts, tok), 0)
    hot0 = expert_iota == e0
    hot1 = expert_iota == e1
    cum_b = dot(ones_where(in_block), upper)
    cum_e = dot(ones_where(jnp.logical_or(hot0, hot1)), upper)
    rank_b = jnp.sum(jnp.where(in_block, cum_b, 0.0), axis=0, keepdims=True).astype(I32)
    rank0 = jnp.sum(jnp.where(hot0, cum_e, 0.0), axis=0, keepdims=True).astype(I32)
    rank1 = jnp.sum(jnp.where(hot1, cum_e, 0.0), axis=0, keepdims=True).astype(I32)
    at_rank = ones_where(lax.broadcasted_iota(I32, (ROW_CAP, tok), 0) == rank_b)
    high6 = jnp.where(in_block, (low // 64).astype(F32), 0.0).astype(BF)
    low6 = jnp.where(in_block, (low % 64).astype(F32), 0.0).astype(BF)
    nt = ((1,), (1,))
    asked = jnp.concatenate(
        [
            dot(high6, at_rank, nt),
            dot(low6, at_rank, nt),
            jnp.zeros((blocks, width - 2 * ROW_CAP), F32),
        ],
        axis=1,
    )
    first = lax.broadcasted_iota(I32, (8, width), 0) == 0
    for b in range(blocks):
        out_ref[b, routed:, :] = jnp.where(first, asked[b : b + 1, :], 0.0).astype(BF)
    slot_b = block * ROW_CAP + rank_b
    slot0 = e0 * CAP + rank0
    slot1 = e1 * CAP + rank1
    position = lax.broadcasted_iota(I32, (1, seq_len), 1)
    valid = jnp.concatenate(
        [jnp.where(position < len_ref[i], 1, 0) for i in range(seqs)], axis=1
    )
    zero = jnp.zeros((1, tok), F32)
    gw0 = gw_ref[0:1, :]
    gw1 = gw_ref[1:2, :]
    rows = jnp.concatenate(
        [
            slot_b.astype(F32),
            valid.astype(F32),
            slot0.astype(F32),
            slot1.astype(F32),
            gw0,
            gw1,
            zero,
            zero,
        ],
        axis=0,
    )
    rows_ref[...] = rows
    cols_ref[...] = rows.T
    d = d_ref[...]
    per = 4
    for b in range(0, blocks, per):
        at = lax.broadcasted_iota(I32, (per * routed, tok), 0) + b * routed
        m0 = at == slot0
        m1 = at == slot1
        moved = dot(ones_where(jnp.logical_or(m0, m1)), d)
        weight = jnp.sum(jnp.where(m0, gw0, jnp.where(m1, gw1, 0.0)), axis=1, keepdims=True)
        out_ref[b : b + per, :routed, :] = (weight * moved).astype(BF).reshape(per, routed, width)


def norm_body(rows_ref, cols_ref, gain_ref, got_ref, emb_ref, out_ref, emb_s, out_s, sems):
    tok, width = emb_s.shape
    blocks, cap, _ = got_ref.shape
    _, routed, _ = out_s.shape
    cols = cols_ref[...]
    rows = rows_ref[...]
    got = got_ref[...].reshape(blocks * cap, width)
    pick = ones_where(
        lax.broadcasted_iota(I32, (tok, blocks * cap), 1) == cols[:, 0:1].astype(I32)
    )
    embedded = jnp.where(cols[:, 1:2] > 0.0, dot(pick, got), 0.0)
    mean_square = jnp.mean(embedded * embedded, axis=1, keepdims=True)
    normed = (embedded * lax.rsqrt(mean_square + EPSILON) * gain_ref[...]).astype(BF)
    slot0 = rows[2:3, :].astype(I32)
    slot1 = rows[3:4, :].astype(I32)
    per = 4
    copies = []
    for n, i in enumerate(range(0, blocks, per)):
        at = lax.broadcasted_iota(I32, (per * routed, tok), 0) + i * routed
        sent = dot(ones_where(jnp.logical_or(at == slot0, at == slot1)), normed).astype(BF)
        out_s[i : i + per] = sent.reshape(per, routed, width)
        copies.append(pltpu.make_async_copy(out_s.at[pl.ds(i, per)], out_ref.at[pl.ds(i, per)], sems.at[n]))
        copies[-1].start()
    emb_s[...] = embedded.astype(BF)
    copies.append(pltpu.make_async_copy(emb_s, emb_ref, sems.at[blocks // per]))
    copies[-1].start()
    for c in copies:
        c.wait()


def expert_rows(ref, j):
    src, _, width = ref.shape
    return ref[:, j * CAP : (j + 1) * CAP, :].reshape(src * CAP, width)


def d_active_body(cot_ref, wd_ref, *outs):
    for j in range(wd_ref.shape[0]):
        cot = expert_rows(cot_ref, j)
        outs[j][...] = dot(cot, wd_ref[j]).astype(BF)
        outs[2 + j][...] = cot.T


def forward_body(j, *refs):
    x_ref, wg_ref, wu_ref, wd_ref, da_ref = refs[:5]
    out_ref, mid, xt, wg, wu, wd, das, outs, sin, sout = refs[-10:]
    _, _, width = outs.shape
    rows = das.shape[0]
    loads = [
        pltpu.make_async_copy(a, b, sin.at[n])
        for n, (a, b) in enumerate(
            ((wg_ref.at[j], wg), (wu_ref.at[j], wu), (wd_ref.at[j], wd), (da_ref, das))
        )
    ]
    for c in loads:
        c.start()
    step = 192
    per = step // CAP
    stores = []
    x = expert_rows(x_ref, j)
    xt[...] = x.T
    for i in range(rows // step):
        r = slice(i * step, (i + 1) * step)
        if i == 0:
            loads[0].wait()
        gate = dot(x[r], wg[...])
        if i == 0:
            loads[1].wait()
        up = dot(x[r], wu[...])
        sigmoid = jax.nn.sigmoid(gate)
        silu = gate * sigmoid
        active = (silu * up).astype(BF)
        if i == 0:
            loads[2].wait()
        out = dot(active, wd[...], ((1,), (1,))).astype(BF)
        outs[i * per : (i + 1) * per] = out.reshape(per, CAP, width)
        here = pl.ds(i * per, per)
        stores.append(
            pltpu.make_async_copy(outs.at[here], out_ref.at[here, pl.ds(j * CAP, CAP)], sout.at[i])
        )
        stores[-1].start()
        if i == 0:
            loads[3].wait()
        da = das[r].astype(F32)
        d_gate = (da * up * sigmoid * (1.0 + gate * (1.0 - sigmoid))).astype(BF)
        d_up = (da * silu).astype(BF)
        for g in range(8):
            c = slice(g * 128, (g + 1) * 128)
            mid[0, g, r, :] = active[:, c]
            mid[1, g, r, :] = d_gate[:, c]
            mid[2, g, r, :] = d_up[:, c]
    for c in stores:
        c.wait()


def products(pre_ref, first, ct_ref, xt_ref, mid_ref):
    for part in range(3):
        lt = (ct_ref if part == 0 else xt_ref)[...]
        for i in (0, 2):
            pair = jnp.concatenate(
                [mid_ref[part, pre_ref[first + i]], mid_ref[part, pre_ref[first + i + 1]]], axis=1
            )
            got = dot(lt, pair)
            yield part, i, got[:, :128]
            yield part, i + 1, got[:, 128:]


def send_body(pre_ref, ct_ref, xt_ref, mid_ref, out_ref):
    for part, i, block in products(pre_ref, 4, ct_ref, xt_ref, mid_ref):
        out_ref[part, i] = block.astype(BF)


def keep_body(
    pre_ref, ct_ref, xt_ref, mid_ref, got_ref, *refs
):
    asend, bsend = refs[2], refs[5]
    ao, an, bo, bn, sems = refs[6:]
    stores = [
        pltpu.make_async_copy(a, b, sems.at[n])
        for n, (a, b) in enumerate(zip((ao, an, bo, bn), (refs[0], refs[1], refs[3], refs[4])))
    ]
    for part, i, block in products(pre_ref, 0, ct_ref, xt_ref, mid_ref):
        total = (block + got_ref[part, i].astype(F32)).astype(BF)
        half = total.shape[0] // 2
        a, b = total[:half], total[half:]
        if i == 0:
            ao[part], bo[part] = a, b
        elif i == 1:
            asend[part, 0], bn[part] = a, b
        elif i == 2:
            asend[part, 1], bsend[part, 1] = a, b
        else:
            an[part], bsend[part, 0] = a, b
    for c in stores:
        c.start()
    for c in stores:
        c.wait()


def add_body(an, ar, bn, br, snd_a, snd_b):
    for keep, got, snd in ((an, ar, snd_a), (bn, br, snd_b)):
        snd[...] = (keep[...].astype(F32) + got[:, 1].astype(F32)).astype(BF)


def final_body(*refs):
    ins, outs = refs[:6], refs[-3:]
    for h in range(2):
        own, got, last = ins[3 * h : 3 * h + 3]
        for part, ref in enumerate(outs):
            half = ref.shape[1] // 2
            total = own[part].astype(F32) + got[part, 0].astype(F32) + last[part].astype(F32)
            ref[0, h * half : (h + 1) * half] = total


def combine_body(cols_ref, emb_ref, ret_ref, out_ref):
    tok = out_ref.shape[0]
    blocks, routed, width = ret_ref.shape
    cols = cols_ref[...]
    ret = ret_ref[...].reshape(blocks * routed, width)
    at = lax.broadcasted_iota(I32, (tok, blocks * routed), 1)
    first = dot(ones_where(at == cols[:, 2:3].astype(I32)), ret)
    second = dot(ones_where(at == cols[:, 3:4].astype(I32)), ret)
    mixed = emb_ref[...].astype(F32) + (cols[:, 4:5] * first + cols[:, 5:6] * second)
    out_ref[...] = mixed.astype(BF)


def exchange(x):
    return lax.all_to_all(x, "ex", split_axis=0, concat_axis=0, tiled=True)


def layer(
    item_ids, lengths, expert_ids, gate_weights, table, norm_gain, w_gate, w_up, w_down, d_out
):
    ex_count = lax.axis_size("ex")
    seqs_here, seq_len = item_ids.shape
    tok = seqs_here * seq_len
    width = table.shape[1]
    exp_here, _, ff = w_gate.shape
    routed = exp_here * CAP
    rows_e = ex_count * CAP
    vmem = pl.BlockSpec(memory_space=pltpu.VMEM)
    smem = pl.BlockSpec(memory_space=pltpu.SMEM)
    hbm = pl.BlockSpec(memory_space=pltpu.HBM)
    dma = pltpu.SemaphoreType.DMA

    outbound, rows, cols = call(
        index_body,
        (
            shape((ex_count, routed + 8, width), BF),
            shape((8, tok), F32),
            shape((tok, 8), F32),
        ),
        56,
        in_specs=[smem] + [vmem] * 4,
        out_specs=(vmem,) * 3,
    )(lengths, item_ids, expert_ids.T, gate_weights.T, d_out)
    inbound = exchange(outbound)
    asked = inbound[:, routed, : 2 * ROW_CAP].astype(F32)
    asked = (asked[:, :ROW_CAP] * 64.0 + asked[:, ROW_CAP:]).astype(I32)
    picked = jnp.take(table, asked.reshape(-1), axis=0, mode="clip")
    got = exchange(picked.reshape(ex_count, ROW_CAP, width))
    embedded, send_rows = call(
        norm_body,
        (pltpu.HBM((tok, width), BF), pltpu.HBM((ex_count, routed, width), BF)),
        14,
        in_specs=[vmem] * 4,
        out_specs=(hbm,) * 2,
        scratch_shapes=[
            pltpu.VMEM((tok, width), BF),
            pltpu.VMEM((ex_count, routed, width), BF),
            dma((5,)),
        ],
    )(rows, cols, norm_gain[None, :], got)
    in_rows = exchange(send_rows)
    turned = shape((width, rows_e), BF)
    *d_active, ct0, ct1 = call(
        d_active_body,
        (shape((rows_e, ff), BF),) * exp_here + (turned,) * exp_here,
        56,
        in_specs=[vmem] * 2,
        out_specs=(vmem,) * (2 * exp_here),
    )(*stay(inbound, w_down))

    me = lax.axis_index("grp")
    place = jnp.arange(8, dtype=I32)
    pre = jnp.bitwise_xor(me // 2, place % 4) * 2 + jnp.bitwise_xor(me % 2, place // 4)
    core = [(g, g ^ 1) for g in range(8)]
    near1 = [(g, g ^ 2) for g in range(8)]
    near3 = [(g, g ^ 6) for g in range(8)]

    def forward(j, back):
        return call(
            lambda *refs: forward_body(j, *refs),
            (
                pltpu.HBM((ex_count, routed, width), BF),
                shape((3, 8, rows_e, 128), BF),
                turned,
            ),
            14,
            in_specs=[vmem] + [hbm] * (4 + len(back)),
            out_specs=(hbm, vmem, vmem),
            input_output_aliases={5: 0} if back else {},
            scratch_shapes=[
                pltpu.VMEM((width, ff), BF),
                pltpu.VMEM((width, ff), BF),
                pltpu.VMEM((width, ff), BF),
                pltpu.VMEM((rows_e, ff), BF),
                pltpu.VMEM((ex_count, CAP, width), BF),
                dma((4,)),
                dma((4,)),
            ],
        )(in_rows, *stay(w_gate, w_up, w_down, d_active[j], *back))

    def send(j, pre, mid, xt):
        sent = call(
            send_body,
            shape((3, 4, width, 128), BF),
            6,
            in_specs=[smem] + [vmem] * 3,
            out_specs=vmem,
        )(pre, (ct0, ct1)[j], xt, mid)
        return sent, lax.ppermute(sent, "grp", core)

    piece = shape((3, width // 2, 128), BF)
    own = pltpu.HBM((3, width // 2, 128), BF)
    pair = shape((3, 2, width // 2, 128), BF)

    def keep(j, pre, mid, xt, crossed):
        ao, an, asend, bo, bn, bsend = call(
            keep_body,
            (own, own, pair) * 2,
            6,
            in_specs=[smem] + [vmem] * 4,
            out_specs=(hbm, hbm, vmem) * 2,
            scratch_shapes=[pltpu.VMEM((3, width // 2, 128), BF)] * 4 + [dma((4,))],
        )(pre, (ct0, ct1)[j], xt, mid, crossed)
        ar = lax.ppermute(asend, "grp", near1)
        br = lax.ppermute(bsend, "grp", near3)
        return ao, an, ar, bo, bn, br

    def add(ao, an, ar, bo, bn, br):
        snd_a, snd_b = call(
            add_body, (piece,) * 2, 6, in_specs=[vmem] * 4, out_specs=(vmem,) * 2
        )(an, ar, bn, br)
        a_last = lax.ppermute(snd_a, "grp", near3)
        b_last = lax.ppermute(snd_b, "grp", near1)
        return ao, ar, a_last, bo, br, b_last

    def final(j, pieces, grads):
        return call(
            final_body,
            (shape((exp_here, width, 128), F32),) * 3,
            8,
            grid=(1,),
            in_specs=[vmem] * 6 + [hbm] * len(grads),
            out_specs=(pl.BlockSpec((1, width, 128), lambda _, j=j: (j, 0, 0)),) * 3,
            input_output_aliases={6 + i: i for i in range(3)} if grads else {},
        )(*pieces, *grads)

    bar = lax.optimization_barrier
    back, mid0, xt0 = forward(0, ())
    sent0, crossed0 = send(0, pre, mid0, xt0)
    back, _ = bar((back, sent0))
    back, mid1, xt1 = forward(1, (back,))
    sent1, crossed1 = send(1, pre, mid1, xt1)
    pre0, _ = bar((pre, sent1))
    kept0 = keep(0, pre0, mid0, xt0, crossed0)
    pre1, _ = bar((pre, kept0[0]))
    kept1 = keep(1, pre1, mid1, xt1, crossed1)
    back, _ = bar((back, kept1[0]))
    returned = exchange(back)
    grads = final(0, add(*kept0), ())
    grad_down, grad_gate, grad_up = final(1, add(*kept1), grads)
    output = call(
        combine_body, shape((tok, width), BF), 12, in_specs=[vmem] * 3, out_specs=vmem
    )(cols, embedded, returned)
    return (output, grad_gate, grad_up, grad_down)


def solution(mesh):
    placed = (
        P(("grp", "ex"), None),
        P(("grp", "ex")),
        P(("grp", "ex"), None),
        P(("grp", "ex"), None),
        P("ex", None),
        P(),
        P("ex", None, None),
        P("ex", None, None),
        P("ex", None, None),
        P(("grp", "ex"), None),
    )
    return jax.shard_map(
        layer,
        mesh=mesh,
        in_specs=placed,
        out_specs=(
            P(("grp", "ex"), None),
            P("ex", None, "grp"),
            P("ex", None, "grp"),
            P("ex", None, "grp"),
        ),
        check_vma=False,
    )
```

```python
import jax
import jax.numpy as jnp
from jax import lax
from jax.experimental import pallas as pl
from jax.experimental.pallas import tpu as pltpu
from jax.sharding import PartitionSpec as P


CAP = 48
ROW_CAP = 128
EPSILON = 1e-06
BF = jnp.bfloat16
F32 = jnp.float32
I32 = jnp.int32


def dot(a, b, dims=((1,), (0,))):
    return lax.dot_general(a, b, (dims, ((), ())), preferred_element_type=F32)


def ones_where(mask):
    return jnp.where(mask, 1.0, 0.0).astype(BF)


def shape(dims, dtype):
    return jax.ShapeDtypeStruct(dims, dtype)


def stay(*arrays):
    return [pltpu.with_memory_space_constraint(x, pltpu.HBM) for x in arrays]


def call(body, out_shape, mib, **kw):
    return pl.pallas_call(
        body,
        out_shape=out_shape,
        compiler_params=pltpu.CompilerParams(vmem_limit_bytes=mib * 1024 * 1024),
        **kw,
    )


def index_body(len_ref, ids_ref, exp_ref, gw_ref, d_ref, out_ref, rows_ref, cols_ref):
    seqs, seq_len = ids_ref.shape
    tok = seqs * seq_len
    blocks = out_ref.shape[0]
    width = d_ref.shape[1]
    routed = out_ref.shape[1] - 8
    experts = blocks * routed // CAP
    ids = jnp.concatenate([ids_ref[i : i + 1, :] for i in range(seqs)], axis=1)
    upper = ones_where(
        lax.broadcasted_iota(I32, (tok, tok), 0) < lax.broadcasted_iota(I32, (tok, tok), 1)
    )
    low = ids % 4096
    block = ids // 4096
    in_block = lax.broadcasted_iota(I32, (blocks, tok), 0) == block
    e0 = exp_ref[0:1, :]
    e1 = exp_ref[1:2, :]
    expert_iota = lax.broadcasted_iota(I32, (experts, tok), 0)
    hot0 = expert_iota == e0
    hot1 = expert_iota == e1
    cum_b = dot(ones_where(in_block), upper)
    cum_e = dot(ones_where(jnp.logical_or(hot0, hot1)), upper)
    rank_b = jnp.sum(jnp.where(in_block, cum_b, 0.0), axis=0, keepdims=True).astype(I32)
    rank0 = jnp.sum(jnp.where(hot0, cum_e, 0.0), axis=0, keepdims=True).astype(I32)
    rank1 = jnp.sum(jnp.where(hot1, cum_e, 0.0), axis=0, keepdims=True).astype(I32)
    at_rank = ones_where(lax.broadcasted_iota(I32, (ROW_CAP, tok), 0) == rank_b)
    high6 = jnp.where(in_block, (low // 64).astype(F32), 0.0).astype(BF)
    low6 = jnp.where(in_block, (low % 64).astype(F32), 0.0).astype(BF)
    nt = ((1,), (1,))
    asked = jnp.concatenate(
        [
            dot(high6, at_rank, nt),
            dot(low6, at_rank, nt),
            jnp.zeros((blocks, width - 2 * ROW_CAP), F32),
        ],
        axis=1,
    )
    first = lax.broadcasted_iota(I32, (8, width), 0) == 0
    for b in range(blocks):
        out_ref[b, routed:, :] = jnp.where(first, asked[b : b + 1, :], 0.0).astype(BF)
    slot_b = block * ROW_CAP + rank_b
    slot0 = e0 * CAP + rank0
    slot1 = e1 * CAP + rank1
    position = lax.broadcasted_iota(I32, (1, seq_len), 1)
    valid = jnp.concatenate(
        [jnp.where(position < len_ref[i], 1, 0) for i in range(seqs)], axis=1
    )
    zero = jnp.zeros((1, tok), F32)
    gw0 = gw_ref[0:1, :]
    gw1 = gw_ref[1:2, :]
    rows = jnp.concatenate(
        [
            slot_b.astype(F32),
            valid.astype(F32),
            slot0.astype(F32),
            slot1.astype(F32),
            gw0,
            gw1,
            zero,
            zero,
        ],
        axis=0,
    )
    rows_ref[...] = rows
    cols_ref[...] = rows.T
    d = d_ref[...]
    per = 4
    for b in range(0, blocks, per):
        at = lax.broadcasted_iota(I32, (per * routed, tok), 0) + b * routed
        m0 = at == slot0
        m1 = at == slot1
        moved = dot(ones_where(jnp.logical_or(m0, m1)), d)
        weight = jnp.sum(jnp.where(m0, gw0, jnp.where(m1, gw1, 0.0)), axis=1, keepdims=True)
        out_ref[b : b + per, :routed, :] = (weight * moved).astype(BF).reshape(per, routed, width)


def norm_body(rows_ref, cols_ref, gain_ref, got_ref, emb_ref, out_ref, emb_s, out_s, sems):
    tok, width = emb_s.shape
    blocks, cap, _ = got_ref.shape
    _, routed, _ = out_s.shape
    cols = cols_ref[...]
    rows = rows_ref[...]
    got = got_ref[...].reshape(blocks * cap, width)
    pick = ones_where(
        lax.broadcasted_iota(I32, (tok, blocks * cap), 1) == cols[:, 0:1].astype(I32)
    )
    embedded = jnp.where(cols[:, 1:2] > 0.0, dot(pick, got), 0.0)
    mean_square = jnp.mean(embedded * embedded, axis=1, keepdims=True)
    normed = (embedded * lax.rsqrt(mean_square + EPSILON) * gain_ref[...]).astype(BF)
    slot0 = rows[2:3, :].astype(I32)
    slot1 = rows[3:4, :].astype(I32)
    per = 4
    emb_s[...] = embedded.astype(BF)
    copies = [pltpu.make_async_copy(emb_s, emb_ref, sems.at[blocks // per])]
    copies[0].start()
    for n, i in enumerate(range(0, blocks, per)):
        at = lax.broadcasted_iota(I32, (per * routed, tok), 0) + i * routed
        sent = dot(ones_where(jnp.logical_or(at == slot0, at == slot1)), normed).astype(BF)
        out_s[i : i + per] = sent.reshape(per, routed, width)
        copies.append(pltpu.make_async_copy(out_s.at[pl.ds(i, per)], out_ref.at[pl.ds(i, per)], sems.at[n]))
        copies[-1].start()
    for c in copies:
        c.wait()


def expert_rows(ref, j):
    src, _, width = ref.shape
    return ref[:, j * CAP : (j + 1) * CAP, :].reshape(src * CAP, width)


def columns(pre_ref, w_ref, j, into, sems, first):
    return [
        pltpu.make_async_copy(
            w_ref.at[j, :, pl.ds(pl.multiple_of(pre_ref[p] * 128, 128), 128)],
            into.at[:, pl.ds(p * 128, 128)],
            sems.at[first + p],
        )
        for p in range(8)
    ]


def d_active_body(pre_ref, cot_ref, wd_ref, *refs):
    outs, (wds, sems) = refs[:4], refs[4:]
    experts = wd_ref.shape[0]
    loads = [columns(pre_ref, wd_ref, j, wds.at[j], sems, 8 * j) for j in range(experts)]
    for group in loads:
        for c in group:
            c.start()
    for j in range(experts):
        cot = expert_rows(cot_ref, j)
        outs[2 + j][...] = cot.T
        for c in loads[j]:
            c.wait()
        outs[j][...] = dot(cot, wds[j]).astype(BF)


def expert_body(j, *refs):
    out_s, mid, sin, sout = refs[-4:]
    if j == 0:
        pre_ref, x_ref, wg_ref, wu_ref, wd_ref, da_ref, ct_ref, da_next, ct_next = refs[:9]
        out_ref, keep_ref, xt_ref, sent_ref = refs[9:13]
        nexts = refs[13:18]
        wg, wu, wd, das, cts = refs[18:23]

        def loads_of(e, da, ct, into, base):
            return (
                columns(pre_ref, wg_ref, e, into[0], sin, base),
                columns(pre_ref, wu_ref, e, into[1], sin, base + 8),
                columns(pre_ref, wd_ref, e, into[2], sin, base + 16),
                [pltpu.make_async_copy(da, into[3], sin.at[base + 24])],
                [pltpu.make_async_copy(ct, into[4], sin.at[base + 25])],
            )

        mine = loads_of(0, da_ref, ct_ref, (wg, wu, wd, das, cts), 0)
        later = loads_of(1, da_next, ct_next, nexts, 26)
    else:
        x_ref, wg, wu, wd, das, cts = refs[:6]
        out_ref, keep_ref, xt_ref, sent_ref = refs[7:11]
        mine, later = ((),) * 5, ()
    gates, ups, downs, das_in, cts_in = mine
    outs = out_s
    _, _, width = outs.shape
    rows, ff = das.shape
    half = ff // 2
    for group in mine:
        for c in group:
            c.start()

    def arrive(group, now=True):
        if now:
            for c in group:
                c.wait()

    step = 192
    per = step // CAP
    stores = []
    x = expert_rows(x_ref, j)
    for i in range(rows // step):
        r = slice(i * step, (i + 1) * step)
        arrive(gates, i == 0)
        gate = dot(x[r], wg[...])
        arrive(ups, i == 0)
        up = dot(x[r], wu[...])
        sigmoid = jax.nn.sigmoid(gate)
        silu = gate * sigmoid
        active = (silu * up).astype(BF)
        arrive(downs, i == 0)
        out = dot(active, wd[...], ((1,), (1,))).astype(BF)
        outs[i * per : (i + 1) * per] = out.reshape(per, CAP, width)
        here = pl.ds(i * per, per)
        stores.append(
            pltpu.make_async_copy(outs.at[here], out_ref.at[here, pl.ds(j * CAP, CAP)], sout.at[i])
        )
        stores[-1].start()
        arrive(das_in, i == 0)
        da = das[r].astype(F32)
        d_gate = (da * up * sigmoid * (1.0 + gate * (1.0 - sigmoid))).astype(BF)
        d_up = (da * silu).astype(BF)
        for part, value in enumerate((active, d_gate, d_up)):
            keep_ref[part, r] = value[:, :half]
            mid[part, r] = value[:, half:]
        if i == 0:
            xt_ref[...] = x.T
            for group in later:
                for c in group:
                    c.start()
    arrive(cts_in)
    for part in range(3):
        got = dot((cts if part == 0 else xt_ref)[...], mid[part]).astype(BF)
        for i in range(4):
            sent_ref[part, i] = got[:, i * 128 : (i + 1) * 128]
    for c in stores:
        c.wait()
    for group in later:
        arrive(group)


def keep_body(ct_ref, xt_ref, mid_ref, got_ref, *refs):
    asend, bsend = refs[2], refs[5]
    own = refs[6:10]
    sems = refs[10]
    ao, an, bo, bn = own
    there = (refs[0], refs[1], refs[3], refs[4])
    stores = []
    for part in range(3):
        got = dot((ct_ref if part == 0 else xt_ref)[...], mid_ref[part])
        half = got.shape[0] // 2
        for i in range(4):
            block = got[:, i * 128 : (i + 1) * 128]
            total = (block + got_ref[part, i].astype(F32)).astype(BF)
            a, b = total[:half], total[half:]
            if i == 0:
                ao[part], bo[part] = a, b
            elif i == 1:
                asend[part, 0], bn[part] = a, b
            elif i == 2:
                asend[part, 1], bsend[part, 1] = a, b
            else:
                an[part], bsend[part, 0] = a, b
        for n in range(4):
            stores.append(
                pltpu.make_async_copy(own[n].at[part], there[n].at[part], sems.at[4 * part + n])
            )
            stores[-1].start()
    for c in stores:
        c.wait()


def add_body(an, ar, bn, br, snd_a, snd_b):
    for keep, got, snd in ((an, ar, snd_a), (bn, br, snd_b)):
        snd[...] = (keep[...].astype(F32) + got[:, 1].astype(F32)).astype(BF)


def final_body(*refs):
    ins, outs = refs[:6], refs[-3:]
    for h in range(2):
        own, got, last = ins[3 * h : 3 * h + 3]
        for part, ref in enumerate(outs):
            half = ref.shape[1] // 2
            total = own[part].astype(F32) + got[part, 0].astype(F32) + last[part].astype(F32)
            ref[0, h * half : (h + 1) * half] = total


def combine_body(cols_ref, emb_ref, ret_ref, out_ref):
    tok = out_ref.shape[0]
    blocks, routed, width = ret_ref.shape
    cols = cols_ref[...]
    ret = ret_ref[...].reshape(blocks * routed, width)
    at = lax.broadcasted_iota(I32, (tok, blocks * routed), 1)
    first = dot(ones_where(at == cols[:, 2:3].astype(I32)), ret)
    second = dot(ones_where(at == cols[:, 3:4].astype(I32)), ret)
    mixed = emb_ref[...].astype(F32) + (cols[:, 4:5] * first + cols[:, 5:6] * second)
    out_ref[...] = mixed.astype(BF)


def exchange(x):
    return lax.all_to_all(x, "ex", split_axis=0, concat_axis=0, tiled=True)


def layer(
    item_ids, lengths, expert_ids, gate_weights, table, norm_gain, w_gate, w_up, w_down, d_out
):
    ex_count = lax.axis_size("ex")
    seqs_here, seq_len = item_ids.shape
    tok = seqs_here * seq_len
    width = table.shape[1]
    exp_here, _, ff = w_gate.shape
    routed = exp_here * CAP
    rows_e = ex_count * CAP
    vmem = pl.BlockSpec(memory_space=pltpu.VMEM)
    smem = pl.BlockSpec(memory_space=pltpu.SMEM)
    hbm = pl.BlockSpec(memory_space=pltpu.HBM)
    dma = pltpu.SemaphoreType.DMA

    me = lax.axis_index("grp")
    place = jnp.arange(8, dtype=I32)
    pre = jnp.bitwise_xor(me // 2, place % 4) * 2 + jnp.bitwise_xor(me % 2, place // 4)
    outbound, rows, cols = call(
        index_body,
        (
            shape((ex_count, routed + 8, width), BF),
            shape((8, tok), F32),
            shape((tok, 8), F32),
        ),
        56,
        in_specs=[smem] + [vmem] * 4,
        out_specs=(vmem,) * 3,
    )(lengths, item_ids, expert_ids.T, gate_weights.T, d_out)
    inbound = exchange(outbound)
    asked = inbound[:, routed, : 2 * ROW_CAP].astype(F32)
    asked = (asked[:, :ROW_CAP] * 64.0 + asked[:, ROW_CAP:]).astype(I32)
    picked = jnp.take(table, asked.reshape(-1), axis=0, mode="clip")
    got = exchange(picked.reshape(ex_count, ROW_CAP, width))
    embedded, send_rows = call(
        norm_body,
        (pltpu.HBM((tok, width), BF), pltpu.HBM((ex_count, routed, width), BF)),
        14,
        in_specs=[vmem] * 4,
        out_specs=(hbm,) * 2,
        scratch_shapes=[
            pltpu.VMEM((tok, width), BF),
            pltpu.VMEM((ex_count, routed, width), BF),
            dma((5,)),
        ],
    )(rows, cols, norm_gain[None, :], got)
    in_rows = exchange(send_rows)
    turned = shape((width, rows_e), BF)
    *d_active, ct0, ct1 = call(
        d_active_body,
        (shape((rows_e, ff), BF),) * exp_here + (turned,) * exp_here,
        56,
        in_specs=[smem, vmem, hbm],
        out_specs=(vmem,) * (2 * exp_here),
        scratch_shapes=[pltpu.VMEM((exp_here, width, ff), BF), dma((8 * exp_here,))],
    )(pre, *stay(inbound, w_down))
    core = [(g, g ^ 1) for g in range(8)]
    near1 = [(g, g ^ 2) for g in range(8)]
    near3 = [(g, g ^ 6) for g in range(8)]
    outs = (
        pltpu.HBM((ex_count, routed, width), BF),
        shape((3, rows_e, ff // 2), BF),
        turned,
        shape((3, 4, width, 128), BF),
    )
    fed = [(width, ff), (width, ff), (width, ff), (rows_e, ff), (width, rows_e)]
    work = [
        pltpu.VMEM((ex_count, CAP, width), BF),
        pltpu.VMEM((3, rows_e, ff // 2), BF),
    ]

    def expert0():
        out, mid, xt, sent, *nexts = call(
            lambda *refs: expert_body(0, *refs),
            outs + tuple(shape(d, BF) for d in fed),
            18,
            in_specs=[smem, vmem] + [hbm] * 7,
            out_specs=(hbm,) + (vmem,) * 8,
            scratch_shapes=[pltpu.VMEM(d, BF) for d in fed] + work + [dma((52,)), dma((4,))],
        )(pre, in_rows, *stay(w_gate, w_up, w_down, d_active[0], ct0, d_active[1], ct1))
        return out, mid, xt, sent, lax.ppermute(sent, "grp", core), nexts

    def expert1(back, nexts):
        out, mid, xt, sent = call(
            lambda *refs: expert_body(1, *refs),
            outs,
            12,
            in_specs=[vmem] * 6 + [hbm],
            out_specs=(hbm,) + (vmem,) * 3,
            input_output_aliases={6: 0},
            scratch_shapes=work + [dma((1,)), dma((4,))],
        )(in_rows, *nexts, *stay(back))
        return out, mid, xt, sent, lax.ppermute(sent, "grp", core)

    piece = shape((3, width // 2, 128), BF)
    own = pltpu.HBM((3, width // 2, 128), BF)
    pair = shape((3, 2, width // 2, 128), BF)

    def keep(j, mid, xt, crossed):
        ao, an, asend, bo, bn, bsend = call(
            keep_body,
            (own, own, pair) * 2,
            6,
            in_specs=[vmem] * 4,
            out_specs=(hbm, hbm, vmem) * 2,
            scratch_shapes=[pltpu.VMEM((3, width // 2, 128), BF)] * 4 + [dma((12,))],
        )((ct0, ct1)[j], xt, mid, crossed)
        ar = lax.ppermute(asend, "grp", near1)
        br = lax.ppermute(bsend, "grp", near3)
        return ao, an, ar, bo, bn, br

    def add(ao, an, ar, bo, bn, br):
        snd_a, snd_b = call(
            add_body, (piece,) * 2, 6, in_specs=[vmem] * 4, out_specs=(vmem,) * 2
        )(*stay(an), ar, *stay(bn), br)
        a_last = lax.ppermute(snd_a, "grp", near3)
        b_last = lax.ppermute(snd_b, "grp", near1)
        return ao, ar, a_last, bo, br, b_last

    def final(j, pieces, grads):
        return call(
            final_body,
            (shape((exp_here, width, 128), F32),) * 3,
            8,
            grid=(1,),
            in_specs=[vmem] * 6 + [hbm] * len(grads),
            out_specs=(pl.BlockSpec((1, width, 128), lambda _, j=j: (j, 0, 0)),) * 3,
            input_output_aliases={6 + i: i for i in range(3)} if grads else {},
        )(*pieces, *grads)

    bar = lax.optimization_barrier
    back, mid0, xt0, sent0, crossed0, nexts = expert0()
    back, _ = bar((back, sent0))
    back, mid1, xt1, sent1, crossed1 = expert1(back, nexts)
    ct1 = nexts[4]
    mid0, _ = bar((mid0, sent1))
    kept0 = keep(0, mid0, xt0, crossed0)
    xt1, _ = bar((xt1, kept0[0]))
    kept1 = keep(1, mid1, xt1, crossed1)
    back, _ = bar((back, kept1[0]))
    returned = exchange(back)
    grads = final(0, add(*kept0), ())
    grad_down, grad_gate, grad_up = final(1, add(*kept1), grads)
    output = call(
        combine_body, shape((tok, width), BF), 12, in_specs=[vmem] * 3, out_specs=vmem
    )(cols, embedded, returned)
    return (output, grad_gate, grad_up, grad_down)


def solution(mesh):
    placed = (
        P(("grp", "ex"), None),
        P(("grp", "ex")),
        P(("grp", "ex"), None),
        P(("grp", "ex"), None),
        P("ex", None),
        P(),
        P("ex", None, None),
        P("ex", None, None),
        P("ex", None, None),
        P(("grp", "ex"), None),
    )
    return jax.shard_map(
        layer,
        mesh=mesh,
        in_specs=placed,
        out_specs=(
            P(("grp", "ex"), None),
            P("ex", None, "grp"),
            P("ex", None, "grp"),
            P("ex", None, "grp"),
        ),
        check_vma=False,
    )
```

```python
import jax
import jax.numpy as jnp
from jax import lax
from jax.experimental import pallas as pl
from jax.experimental.pallas import tpu as pltpu
from jax.sharding import PartitionSpec as P


CAP = 48
ROW_CAP = 128
EPSILON = 1e-06
BF = jnp.bfloat16
F32 = jnp.float32
I32 = jnp.int32


def dot(a, b, dims=((1,), (0,))):
    return lax.dot_general(a, b, (dims, ((), ())), preferred_element_type=F32)


def ones_where(mask):
    return jnp.where(mask, 1.0, 0.0).astype(BF)


def shape(dims, dtype):
    return jax.ShapeDtypeStruct(dims, dtype)


def stay(*arrays):
    return [pltpu.with_memory_space_constraint(x, pltpu.HBM) for x in arrays]


def call(body, out_shape, mib, **kw):
    return pl.pallas_call(
        body,
        out_shape=out_shape,
        compiler_params=pltpu.CompilerParams(vmem_limit_bytes=mib * 1024 * 1024),
        **kw,
    )


def index_body(len_ref, ids_ref, exp_ref, gw_ref, d_ref, out_ref, rows_ref, cols_ref):
    seqs, seq_len = ids_ref.shape
    tok = seqs * seq_len
    blocks = out_ref.shape[0]
    width = d_ref.shape[1]
    routed = out_ref.shape[1] - 8
    experts = blocks * routed // CAP
    ids = jnp.concatenate([ids_ref[i : i + 1, :] for i in range(seqs)], axis=1)
    upper = ones_where(
        lax.broadcasted_iota(I32, (tok, tok), 0) < lax.broadcasted_iota(I32, (tok, tok), 1)
    )
    low = ids % 4096
    block = ids // 4096
    in_block = lax.broadcasted_iota(I32, (blocks, tok), 0) == block
    e0 = exp_ref[0:1, :]
    e1 = exp_ref[1:2, :]
    expert_iota = lax.broadcasted_iota(I32, (experts, tok), 0)
    hot0 = expert_iota == e0
    hot1 = expert_iota == e1
    cum_b = dot(ones_where(in_block), upper)
    cum_e = dot(ones_where(jnp.logical_or(hot0, hot1)), upper)
    rank_b = jnp.sum(jnp.where(in_block, cum_b, 0.0), axis=0, keepdims=True).astype(I32)
    rank0 = jnp.sum(jnp.where(hot0, cum_e, 0.0), axis=0, keepdims=True).astype(I32)
    rank1 = jnp.sum(jnp.where(hot1, cum_e, 0.0), axis=0, keepdims=True).astype(I32)
    at_rank = ones_where(lax.broadcasted_iota(I32, (ROW_CAP, tok), 0) == rank_b)
    high6 = jnp.where(in_block, (low // 64).astype(F32), 0.0).astype(BF)
    low6 = jnp.where(in_block, (low % 64).astype(F32), 0.0).astype(BF)
    nt = ((1,), (1,))
    asked = jnp.concatenate(
        [
            dot(high6, at_rank, nt),
            dot(low6, at_rank, nt),
            jnp.zeros((blocks, width - 2 * ROW_CAP), F32),
        ],
        axis=1,
    )
    first = lax.broadcasted_iota(I32, (8, width), 0) == 0
    for b in range(blocks):
        out_ref[b, routed:, :] = jnp.where(first, asked[b : b + 1, :], 0.0).astype(BF)
    slot_b = block * ROW_CAP + rank_b
    slot0 = e0 * CAP + rank0
    slot1 = e1 * CAP + rank1
    position = lax.broadcasted_iota(I32, (1, seq_len), 1)
    valid = jnp.concatenate(
        [jnp.where(position < len_ref[i], 1, 0) for i in range(seqs)], axis=1
    )
    zero = jnp.zeros((1, tok), F32)
    gw0 = gw_ref[0:1, :]
    gw1 = gw_ref[1:2, :]
    rows = jnp.concatenate(
        [
            slot_b.astype(F32),
            valid.astype(F32),
            slot0.astype(F32),
            slot1.astype(F32),
            gw0,
            gw1,
            zero,
            zero,
        ],
        axis=0,
    )
    rows_ref[...] = rows
    cols_ref[...] = rows.T
    d = d_ref[...]
    per = 4
    for b in range(0, blocks, per):
        at = lax.broadcasted_iota(I32, (per * routed, tok), 0) + b * routed
        m0 = at == slot0
        m1 = at == slot1
        moved = dot(ones_where(jnp.logical_or(m0, m1)), d)
        weight = jnp.sum(jnp.where(m0, gw0, jnp.where(m1, gw1, 0.0)), axis=1, keepdims=True)
        out_ref[b : b + per, :routed, :] = (weight * moved).astype(BF).reshape(per, routed, width)


def norm_body(rows_ref, cols_ref, gain_ref, got_ref, emb_ref, out_ref, emb_s, out_s, sems):
    tok, width = emb_s.shape
    blocks, cap, _ = got_ref.shape
    _, routed, _ = out_s.shape
    cols = cols_ref[...]
    rows = rows_ref[...]
    got = got_ref[...].reshape(blocks * cap, width)
    pick = ones_where(
        lax.broadcasted_iota(I32, (tok, blocks * cap), 1) == cols[:, 0:1].astype(I32)
    )
    embedded = jnp.where(cols[:, 1:2] > 0.0, dot(pick, got), 0.0)
    mean_square = jnp.mean(embedded * embedded, axis=1, keepdims=True)
    normed = (embedded * lax.rsqrt(mean_square + EPSILON) * gain_ref[...]).astype(BF)
    slot0 = rows[2:3, :].astype(I32)
    slot1 = rows[3:4, :].astype(I32)
    per = 4
    emb_s[...] = embedded.astype(BF)
    copies = [pltpu.make_async_copy(emb_s, emb_ref, sems.at[blocks // per])]
    copies[0].start()
    for n, i in enumerate(range(0, blocks, per)):
        at = lax.broadcasted_iota(I32, (per * routed, tok), 0) + i * routed
        sent = dot(ones_where(jnp.logical_or(at == slot0, at == slot1)), normed).astype(BF)
        out_s[i : i + per] = sent.reshape(per, routed, width)
        copies.append(pltpu.make_async_copy(out_s.at[pl.ds(i, per)], out_ref.at[pl.ds(i, per)], sems.at[n]))
        copies[-1].start()
    for c in copies:
        c.wait()


def expert_rows(ref, j):
    src, _, width = ref.shape
    return ref[:, j * CAP : (j + 1) * CAP, :].reshape(src * CAP, width)


def columns(pre_ref, w_ref, j, into, sems, first):
    return [
        pltpu.make_async_copy(
            w_ref.at[j, :, pl.ds(pl.multiple_of(pre_ref[p] * 128, 128), 128)],
            into.at[:, pl.ds(p * 128, 128)],
            sems.at[first + p],
        )
        for p in range(8)
    ]


def d_active_body(pre_ref, cot_ref, wd_ref, wg_ref, wu_ref, *refs):
    outs, placed, (wds, wgs, wus, sems, sout) = refs[:4], refs[4:7], refs[7:]
    experts = wd_ref.shape[0]
    moves = ((wd_ref, wds), (wg_ref, wgs), (wu_ref, wus))
    loads = [
        [
            c
            for j in range(experts)
            for c in columns(pre_ref, ref, j, into.at[j], sems, 8 * (experts * n + j))
        ]
        for n, (ref, into) in enumerate(moves)
    ]
    stores = [
        pltpu.make_async_copy(into, placed[n], sout.at[n]) for n, (_, into) in enumerate(moves)
    ]
    for group in loads:
        for c in group:
            c.start()
    for n in range(3):
        for c in loads[n]:
            c.wait()
        stores[n].start()
    for j in range(experts):
        cot = expert_rows(cot_ref, j)
        outs[2 + j][...] = cot.T
        outs[j][...] = dot(cot, wds[j]).astype(BF)
    for c in stores:
        c.wait()


def expert_body(j, *refs):
    out_s, mid, sin, sout = refs[-4:]
    if j == 0:
        x_ref, wg_ref, wu_ref, wd_ref, da_ref, ct_ref, da_next, ct_next = refs[:8]
        out_ref, keep_ref, xt_ref, sent_ref = refs[8:12]
        nexts = refs[12:17]
        wg, wu, wd, das, cts = refs[17:22]

        def loads_of(e, da, ct, into, base):
            pairs = zip((wg_ref.at[e], wu_ref.at[e], wd_ref.at[e], da, ct), into)
            return [
                [pltpu.make_async_copy(a, b, sin.at[base + n])] for n, (a, b) in enumerate(pairs)
            ]

        mine = loads_of(0, da_ref, ct_ref, (wg, wu, wd, das, cts), 0)
        later = loads_of(1, da_next, ct_next, nexts, 5)
    else:
        x_ref, wg, wu, wd, das, cts = refs[:6]
        out_ref, keep_ref, xt_ref, sent_ref = refs[7:11]
        mine, later = ((),) * 5, ()
    gates, ups, downs, das_in, cts_in = mine
    outs = out_s
    _, _, width = outs.shape
    rows, ff = das.shape
    half = ff // 2
    for group in mine:
        for c in group:
            c.start()

    def arrive(group, now=True):
        if now:
            for c in group:
                c.wait()

    step = 192
    per = step // CAP
    stores = []
    x = expert_rows(x_ref, j)
    if j == 0:
        xt_ref[...] = x.T
    for i in range(rows // step):
        r = slice(i * step, (i + 1) * step)
        arrive(gates, i == 0)
        gate = dot(x[r], wg[...])
        arrive(ups, i == 0)
        up = dot(x[r], wu[...])
        sigmoid = jax.nn.sigmoid(gate)
        silu = gate * sigmoid
        active = (silu * up).astype(BF)
        arrive(downs, i == 0)
        out = dot(active, wd[...], ((1,), (1,))).astype(BF)
        outs[i * per : (i + 1) * per] = out.reshape(per, CAP, width)
        here = pl.ds(i * per, per)
        stores.append(
            pltpu.make_async_copy(outs.at[here], out_ref.at[here, pl.ds(j * CAP, CAP)], sout.at[i])
        )
        stores[-1].start()
        arrive(das_in, i == 0)
        da = das[r].astype(F32)
        d_gate = (da * up * sigmoid * (1.0 + gate * (1.0 - sigmoid))).astype(BF)
        d_up = (da * silu).astype(BF)
        for part, value in enumerate((active, d_gate, d_up)):
            keep_ref[part, r] = value[:, :half]
            mid[part, r] = value[:, half:]
        if i == 0:
            if j != 0:
                xt_ref[...] = x.T
            for group in later:
                for c in group:
                    c.start()
    arrive(cts_in)
    for part in range(3):
        got = dot((cts if part == 0 else xt_ref)[...], mid[part]).astype(BF)
        for i in range(4):
            sent_ref[part, i] = got[:, i * 128 : (i + 1) * 128]
    for c in stores:
        c.wait()
    for group in later:
        arrive(group)


def keep_body(leaves, ct_ref, xt_ref, mid_ref, got_ref, *refs):
    outs, staged, sems = refs[:6], list(refs[6:-1]), refs[-1]
    stage = [staged.pop(0) if leaves[k] else outs[k] for k in range(6)]
    ao, an, asend, bo, bn, bsend = stage
    stores = []
    for part in range(3):
        got = dot((ct_ref if part == 0 else xt_ref)[...], mid_ref[part])
        half = got.shape[0] // 2
        for i in range(4):
            block = got[:, i * 128 : (i + 1) * 128]
            total = (block + got_ref[part, i].astype(F32)).astype(BF)
            a, b = total[:half], total[half:]
            if i == 0:
                ao[part], bo[part] = a, b
            elif i == 1:
                asend[part, 0], bn[part] = a, b
            elif i == 2:
                asend[part, 1], bsend[part, 1] = a, b
            else:
                an[part], bsend[part, 0] = a, b
        for k in range(6):
            if leaves[k]:
                stores.append(
                    pltpu.make_async_copy(
                        stage[k].at[part], outs[k].at[part], sems.at[6 * part + k]
                    )
                )
                stores[-1].start()
    for c in stores:
        c.wait()


def add_body(an, ar, bn, br, snd_a, snd_b):
    for keep, got, snd in ((an, ar, snd_a), (bn, br, snd_b)):
        snd[...] = (keep[...].astype(F32) + got[:, 1].astype(F32)).astype(BF)


def final_body(*refs):
    ins, outs = refs[:6], refs[-3:]
    for h in range(2):
        own, got, last = ins[3 * h : 3 * h + 3]
        for part, ref in enumerate(outs):
            half = ref.shape[1] // 2
            total = own[part].astype(F32) + got[part, 0].astype(F32) + last[part].astype(F32)
            ref[0, h * half : (h + 1) * half] = total


def combine_body(cols_ref, emb_ref, ret_ref, out_ref):
    tok = out_ref.shape[0]
    blocks, routed, width = ret_ref.shape
    cols = cols_ref[...]
    ret = ret_ref[...].reshape(blocks * routed, width)
    at = lax.broadcasted_iota(I32, (tok, blocks * routed), 1)
    first = dot(ones_where(at == cols[:, 2:3].astype(I32)), ret)
    second = dot(ones_where(at == cols[:, 3:4].astype(I32)), ret)
    mixed = emb_ref[...].astype(F32) + (cols[:, 4:5] * first + cols[:, 5:6] * second)
    out_ref[...] = mixed.astype(BF)


def exchange(x):
    return lax.all_to_all(x, "ex", split_axis=0, concat_axis=0, tiled=True)


def layer(
    item_ids, lengths, expert_ids, gate_weights, table, norm_gain, w_gate, w_up, w_down, d_out
):
    ex_count = lax.axis_size("ex")
    seqs_here, seq_len = item_ids.shape
    tok = seqs_here * seq_len
    width = table.shape[1]
    exp_here, _, ff = w_gate.shape
    routed = exp_here * CAP
    rows_e = ex_count * CAP
    vmem = pl.BlockSpec(memory_space=pltpu.VMEM)
    smem = pl.BlockSpec(memory_space=pltpu.SMEM)
    hbm = pl.BlockSpec(memory_space=pltpu.HBM)
    dma = pltpu.SemaphoreType.DMA

    me = lax.axis_index("grp")
    place = jnp.arange(8, dtype=I32)
    pre = jnp.bitwise_xor(me // 2, place % 4) * 2 + jnp.bitwise_xor(me % 2, place // 4)
    outbound, rows, cols = call(
        index_body,
        (
            pltpu.VMEM((ex_count, routed + 8, width), BF),
            shape((8, tok), F32),
            shape((tok, 8), F32),
        ),
        56,
        in_specs=[smem] + [vmem] * 4,
        out_specs=(vmem,) * 3,
    )(lengths, item_ids, expert_ids.T, gate_weights.T, d_out)
    inbound = exchange(outbound)
    asked = inbound[:, routed, : 2 * ROW_CAP].astype(F32)
    asked = (asked[:, :ROW_CAP] * 64.0 + asked[:, ROW_CAP:]).astype(I32)
    picked = jnp.take(table, asked.reshape(-1), axis=0, mode="clip")
    got = exchange(picked.reshape(ex_count, ROW_CAP, width))
    embedded, send_rows = call(
        norm_body,
        (pltpu.HBM((tok, width), BF), pltpu.HBM((ex_count, routed, width), BF)),
        14,
        in_specs=[vmem] * 4,
        out_specs=(hbm,) * 2,
        scratch_shapes=[
            pltpu.VMEM((tok, width), BF),
            pltpu.VMEM((ex_count, routed, width), BF),
            dma((5,)),
        ],
    )(rows, cols, norm_gain[None, :], got)
    in_rows = exchange(send_rows)
    turned = shape((width, rows_e), BF)
    weights = (exp_here, width, ff)
    *d_active, ct0, ct1, wd_placed, wg_placed, wu_placed = call(
        d_active_body,
        (shape((rows_e, ff), BF),) * exp_here
        + (turned,) * exp_here
        + (pltpu.HBM(weights, BF),) * 3,
        56,
        in_specs=[smem, vmem] + [hbm] * 3,
        out_specs=(vmem,) * (2 * exp_here) + (hbm,) * 3,
        scratch_shapes=[pltpu.VMEM(weights, BF)] * 3 + [dma((24 * exp_here,)), dma((3,))],
    )(pre, *stay(inbound, w_down, w_gate, w_up))
    core = [(g, g ^ 1) for g in range(8)]
    near1 = [(g, g ^ 2) for g in range(8)]
    near3 = [(g, g ^ 6) for g in range(8)]
    outs = (
        pltpu.HBM((ex_count, routed, width), BF),
        shape((3, rows_e, ff // 2), BF),
        turned,
        shape((3, 4, width, 128), BF),
    )
    fed = [(width, ff), (width, ff), (width, ff), (rows_e, ff), (width, rows_e)]
    work = [
        pltpu.VMEM((ex_count, CAP, width), BF),
        pltpu.VMEM((3, rows_e, ff // 2), BF),
    ]

    def expert0():
        out, mid, xt, sent, *nexts = call(
            lambda *refs: expert_body(0, *refs),
            outs + tuple(shape(d, BF) for d in fed),
            18,
            in_specs=[vmem] + [hbm] * 7,
            out_specs=(hbm,) + (vmem,) * 8,
            scratch_shapes=[pltpu.VMEM(d, BF) for d in fed] + work + [dma((10,)), dma((4,))],
        )(in_rows, *stay(wg_placed, wu_placed, wd_placed, d_active[0], ct0, d_active[1], ct1))
        return out, mid, xt, sent, lax.ppermute(sent, "grp", core), nexts

    def expert1(back, nexts):
        out, mid, xt, sent = call(
            lambda *refs: expert_body(1, *refs),
            outs,
            12,
            in_specs=[vmem] * 6 + [hbm],
            out_specs=(hbm,) + (vmem,) * 3,
            input_output_aliases={6: 0},
            scratch_shapes=work + [dma((1,)), dma((4,))],
        )(in_rows, *nexts, *stay(back))
        return out, mid, xt, sent, lax.ppermute(sent, "grp", core)

    piece = shape((3, width // 2, 128), BF)
    own = pltpu.HBM((3, width // 2, 128), BF)

    def keep(j, mid, xt, crossed):
        leaves = (True, True, j == 1) * 2
        dims = ((3, width // 2, 128), (3, width // 2, 128), (3, 2, width // 2, 128)) * 2
        ao, an, asend, bo, bn, bsend = call(
            lambda *refs: keep_body(leaves, *refs),
            tuple(pltpu.HBM(d, BF) if k else shape(d, BF) for d, k in zip(dims, leaves)),
            6,
            in_specs=[vmem] * 4,
            out_specs=tuple(hbm if k else vmem for k in leaves),
            scratch_shapes=[pltpu.VMEM(d, BF) for d, k in zip(dims, leaves) if k] + [dma((18,))],
        )((ct0, ct1)[j], xt, mid, crossed)
        ar = lax.ppermute(asend, "grp", near1)
        br = lax.ppermute(bsend, "grp", near3)
        return ao, an, ar, bo, bn, br

    def add(ao, an, ar, bo, bn, br):
        snd_a, snd_b = call(
            add_body, (piece,) * 2, 6, in_specs=[vmem] * 4, out_specs=(vmem,) * 2
        )(*stay(an), ar, *stay(bn), br)
        a_last = lax.ppermute(snd_a, "grp", near3)
        b_last = lax.ppermute(snd_b, "grp", near1)
        return ao, ar, a_last, bo, br, b_last

    def final(j, pieces, grads):
        return call(
            final_body,
            (shape((exp_here, width, 128), F32),) * 3,
            8,
            grid=(1,),
            in_specs=[vmem] * 6 + [hbm] * len(grads),
            out_specs=(pl.BlockSpec((1, width, 128), lambda _, j=j: (j, 0, 0)),) * 3,
            input_output_aliases={6 + i: i for i in range(3)} if grads else {},
        )(*pieces, *grads)

    bar = lax.optimization_barrier
    back, mid0, xt0, sent0, crossed0, nexts = expert0()
    back, _ = bar((back, sent0))
    back, mid1, xt1, sent1, crossed1 = expert1(back, nexts)
    ct1 = nexts[4]
    mid0, _ = bar((mid0, sent1))
    kept0 = keep(0, mid0, xt0, crossed0)
    xt1, _ = bar((xt1, kept0[0]))
    kept1 = keep(1, mid1, xt1, crossed1)
    back, _ = bar((back, kept1[0]))
    returned = exchange(back)
    grads = final(0, add(*kept0), ())
    grad_down, grad_gate, grad_up = final(1, add(*kept1), grads)
    output = call(
        combine_body, shape((tok, width), BF), 12, in_specs=[vmem] * 3, out_specs=vmem
    )(cols, embedded, returned)
    return (output, grad_gate, grad_up, grad_down)


def solution(mesh):
    placed = (
        P(("grp", "ex"), None),
        P(("grp", "ex")),
        P(("grp", "ex"), None),
        P(("grp", "ex"), None),
        P("ex", None),
        P(),
        P("ex", None, None),
        P("ex", None, None),
        P("ex", None, None),
        P(("grp", "ex"), None),
    )
    return jax.shard_map(
        layer,
        mesh=mesh,
        in_specs=placed,
        out_specs=(
            P(("grp", "ex"), None),
            P("ex", None, "grp"),
            P("ex", None, "grp"),
            P("ex", None, "grp"),
        ),
        check_vma=False,
    )
```
